32 devices in a mesh: row: 8 (over z, x), col: 4 (over y, core).
Axes of the slice: x: 2, y: 2, z: 4, core: 2. Of those that a mesh axis runs over, the one named last changes fastest.
Arguments:
- gradients: bfloat16 [32, 2, 524288], P(('row', 'col')), may hold values from -96 to 96
- master_params: float32 [2, 524288], P(None, ('row', 'col')), may hold values from -0.1 to 0.1
- first_moment: float32 [2, 524288], P(None, ('row', 'col')), may hold values from -3 to 3
- second_moment: float32 [2, 524288], P(None, ('row', 'col')), may hold values from 0.05 to 5
Outputs:
- new_master: float32 [2, 524288], P(None, ('row', 'col'))
- new_first: float32 [2, 524288], P(None, ('row', 'col'))
- new_second: float32 [2, 524288], P(None, ('row', 'col'))
- new_weights: bfloat16 [2, 524288], replicated
The draws below stay inside these ranges and needn't reach their ends.
All inputs are finite; a program needn't handle non-finite values.
Results may differ from the reference program's by a relative error of at most 0.009.
Values may be sent and summed in bfloat16 or wider, within the bound.
No kernel may reach another device: no remote copies, remote signals or barrier semaphores. Data moves between devices by JAX's collectives and lax.ppermute only.
A program may use at most 64 MiB of HBM per device.

```python
import math
import jax
import jax.numpy as jnp
from jax import lax

LAYERS = 2
SLICE = 524288
DEVICES = 32


def spiked(result, rng, source, target, shards_of, factor):
    owner, partner = [(jnp.arange(result.shape[axis_at]) // (result.shape[axis_at] // shards_of)).reshape([-1 if axis == axis_at else 1 for axis in range(result.ndim)]) for axis_at in (source, target)]
    chosen = jax.random.permutation(rng, shards_of)[partner]
    strong = (owner == chosen) | (owner == (partner + shards_of // 2) % shards_of)
    return jnp.where(strong, factor * result, result)


def level_of(own_key, extent, split, smallest, largest):
    factor_of, own = 1.0, jax.random.fold_in(own_key, 6)
    for position, parts in split:
        heights = jnp.exp(jax.random.uniform(jax.random.fold_in(own, position), (parts,), jnp.float32, smallest / len(split), largest / len(split)))
        factor_of = factor_of * jnp.repeat(heights, extent[position] // parts).reshape([-1 if axis == position else 1 for axis in range(len(extent))])
    return factor_of


def gaussian(rng, dims, spread, most, split=(), held_as=jnp.bfloat16):
    result = jax.random.normal(rng, dims, jnp.float32) * spread
    if len(split) > 0:
        result = level_of(rng, dims, split, -0.22, 0.18) * result
    return jnp.clip(result, min=-most, max=most).astype(held_as)


def heavy_noise(own_key, dims, spread, bound, pieces, heavy, kind=jnp.bfloat16):
    drawn = spread * jax.random.normal(own_key, dims, jnp.float32)
    if pieces:
        drawn = drawn * level_of(own_key, dims, pieces, -0.22, 0.18)
    return jnp.clip(spiked(drawn, jax.random.fold_in(own_key, 3), *heavy), -bound, bound).astype(kind)


def setup_inputs(seed: int = 0) -> dict:
    splits = jax.random.split(jax.random.key(seed), 5)
    gradients = heavy_noise(splits[0], (DEVICES, LAYERS, SLICE), 16.0, 96.0, ((0, 32),), (0, 2, 32, 2.75))
    master_params = gaussian(splits[1], (LAYERS, SLICE), 0.025, 0.1, ((1, 32),), jnp.float32)
    first_moment = gaussian(splits[2], (LAYERS, SLICE), 0.5, 3.0, ((1, 32),), jnp.float32)
    second_moment = jnp.clip(jnp.exp(math.log(5.0) - 4.6051702 * jax.random.uniform(splits[3], (LAYERS, SLICE), jnp.float32) ** level_of(splits[3], (LAYERS, SLICE), ((1, 32),), -0.2, 0.2)), 0.05, 5.0)
    return {"gradients": gradients, "master_params": master_params, "first_moment": first_moment, "second_moment": second_moment}


beta_one = 0.9
beta_two = 0.95
learn_rate = 0.001
decay_rate = 0.1
epsilon = 1e-08
adam_step = 10.0

def adam_update(mean_grad, master_params, first_moment, second_moment):
    new_first = beta_one * first_moment + (1.0 - beta_one) * mean_grad
    new_second = beta_two * second_moment + (1.0 - beta_two) * mean_grad * mean_grad
    first_hat = new_first / (1.0 - beta_one ** adam_step)
    second_hat = new_second / (1.0 - beta_two ** adam_step)
    new_master = master_params - learn_rate * (first_hat / (jnp.sqrt(second_hat) + epsilon) + decay_rate * master_params)
    return (new_master, new_first, new_second)

def reference(gradients, master_params, first_moment, second_moment):
    mean_grad = lax.optimization_barrier(jnp.sum(gradients, axis=0, dtype=jnp.float32)) / DEVICES
    new_master, new_first, new_second = adam_update(mean_grad, master_params, first_moment, second_moment)
    return (new_master, new_first, new_second, new_master.astype(jnp.bfloat16))
```

```python
import jax
import jax.numpy as jnp
from jax import lax
from jax.sharding import PartitionSpec as P

beta_one = 0.9
beta_two = 0.95
learn_rate = 0.001
decay_rate = 0.1
epsilon = 1e-08
adam_step = 10.0

AXES = ("row", "col")
LANES = 128
COLOURS = 3


def adam_update(mean_grad, master_params, first_moment, second_moment):
    new_first = beta_one * first_moment + (1.0 - beta_one) * mean_grad
    new_second = beta_two * second_moment + (1.0 - beta_two) * mean_grad * mean_grad
    first_hat = new_first / (1.0 - beta_one**adam_step)
    second_hat = new_second / (1.0 - beta_two**adam_step)
    new_master = master_params - learn_rate * (
        first_hat / (jnp.sqrt(second_hat) + epsilon) + decay_rate * master_params
    )
    return (new_master, new_first, new_second)


def rows_view(x):
    layers, n = x.shape
    return x.reshape(layers, n // LANES, LANES).transpose(1, 0, 2).reshape(-1, LANES)


def layers_view(x, layers):
    return x.reshape(-1, layers, LANES).transpose(1, 0, 2).reshape(layers, -1)


def colour_plan(bits, rows):
    rest = [1, 3, 2][: max(bits - 1, 0)] if bits >= 4 else list(range(1, bits))
    later = [b for b in range(1, bits) if b not in rest]
    count = max(min(COLOURS, len(rest)), 1)
    cuts = [8 * ((rows // 8) * k // count) for k in range(count)] + [rows]
    plan = []
    for k in range(count):
        turned = rest[k:] + rest[:k]
        plan.append((cuts[k], cuts[k + 1], [0] + turned + later))
    return plan


def swap(x, bit, devices):
    return lax.ppermute(x, AXES, [(i, i ^ (1 << bit)) for i in range(devices)])


def shards(gradients, master_params, first_moment, second_moment):
    devices = lax.axis_size("row") * lax.axis_size("col")
    me = lax.axis_index("row") * lax.axis_size("col") + lax.axis_index("col")
    layers = gradients.shape[1]
    bits = devices.bit_length() - 1
    mine = [(me >> b) & 1 for b in range(bits)]
    flat = rows_view(gradients[0])
    rows = flat.shape[0] // devices
    pieces = flat.reshape((2,) * bits + (rows, LANES))
    plan = colour_plan(bits, rows)

    sums = []
    for low, high, order in plan:
        part = pieces[..., low:high, :]
        left = list(range(bits))[::-1]
        for bit in order:
            axis = left.index(bit)
            away = lax.dynamic_index_in_dim(part, 1 - mine[bit], axis, keepdims=False)
            keep = lax.dynamic_index_in_dim(part, mine[bit], axis, keepdims=False)
            came = swap(away.astype(jnp.bfloat16), bit, devices)
            part = keep.astype(jnp.float32) + came.astype(jnp.float32)
            left.remove(bit)
        sums.append(part)
    mean_grad = jnp.concatenate(sums, axis=0) / devices

    new_master, new_first, new_second = adam_update(
        mean_grad, rows_view(master_params), rows_view(first_moment), rows_view(second_moment)
    )
    rounded = new_master.astype(jnp.bfloat16)

    gathered = []
    for low, high, order in plan:
        part = rounded[low:high]
        have = []
        for bit in order[::-1]:
            came = swap(part, bit, devices)
            have.append(bit)
            have.sort(reverse=True)
            axis = have.index(bit)
            part = jnp.where(
                mine[bit] == 0, jnp.stack([part, came], axis), jnp.stack([came, part], axis)
            )
        gathered.append(part)
    new_weights = jnp.concatenate(gathered, axis=-2).reshape(-1, LANES)

    return (
        layers_view(new_master, layers),
        layers_view(new_first, layers),
        layers_view(new_second, layers),
        layers_view(new_weights, layers),
    )


def solution(mesh):
    in_specs = (P(AXES, None, None), P(None, AXES), P(None, AXES), P(None, AXES))
    out_specs = (P(None, AXES), P(None, AXES), P(None, AXES), P())
    return jax.shard_map(shards, mesh=mesh, in_specs=in_specs, out_specs=out_specs, check_vma=False)
```

```python
import jax
import jax.numpy as jnp
from jax import lax
from jax.experimental import pallas as pl
from jax.experimental.pallas import tpu as pltpu
from jax.sharding import PartitionSpec as P

beta_one = 0.9
beta_two = 0.95
learn_rate = 0.001
decay_rate = 0.1
epsilon = 1e-08
adam_step = 10.0

AXES = ("row", "col")
LANES = 128
Y, X, Z = 0, 1, 2
SHARES = (0, 8)
GATHER_GRANT = 52 << 20
ORDERS = (((X, Y, Z), (Y, Z, X)), ((X, Y, Z), (Z, X, Y)))


def adam_update(mean_grad, master_params, first_moment, second_moment):
    new_first = beta_one * first_moment + (1.0 - beta_one) * mean_grad
    new_second = beta_two * second_moment + (1.0 - beta_two) * mean_grad * mean_grad
    first_hat = new_first / (1.0 - beta_one**adam_step)
    second_hat = new_second / (1.0 - beta_two**adam_step)
    new_master = master_params - learn_rate * (
        first_hat / (jnp.sqrt(second_hat) + epsilon) + decay_rate * master_params
    )
    return (new_master, new_first, new_second)


def rows_view(x):
    layers, n = x.shape
    return x.reshape(layers, n // LANES, LANES).transpose(1, 0, 2).reshape(-1, LANES)


def layers_view(x, layers):
    return x.reshape(-1, layers, LANES).transpose(1, 0, 2).reshape(layers, -1)


class Part:
    def __init__(self, low, high, orders):
        self.low, self.high, self.orders = low, high, orders
        self.size = high - low
        self.steps = len(orders[0])
        self.blocks = 1 << self.steps

    def mask(self, team, step):
        return 1 << self.orders[team][step] | 1

    def offset(self, team, position):
        bits = 0
        for step in range(self.steps):
            if position >> (self.steps - 1 - step) & 1:
                bits ^= self.mask(team, step)
        return bits


def parts_of(bits, rows):
    rest = list(range(1, bits))
    if bits < 4:
        return [Part(0, rows, (rest, rest[::-1]))]
    tail = rest[3:]
    cuts = [8 * (rows * share // (8 * 16)) for share in SHARES] + [rows]
    return [
        Part(cuts[k], cuts[k + 1], [[rest[i] for i in order] + tail for order in ORDERS[k]])
        for k in range(len(SHARES))
    ]


def place_index():
    devices = lax.axis_size("row") * lax.axis_size("col")
    me = lax.axis_index("row") * lax.axis_size("col") + lax.axis_index("col")
    team = me
    for bit in range(1, devices.bit_length() - 1):
        team = team ^ (me >> bit)
    return me, team & 1


def piece_of(part, me, team, mine, position):
    first, second = part.offset(0, position), part.offset(1, position)
    if not mine:
        first, second = second, first
    return (me if mine else me ^ 1) ^ jnp.where(team == 0, first, second)


def gather_pieces(flat, parts, rows):
    def body(flat_ref, *refs):
        me, team = place_index()
        sems = refs[-1]
        copies = []
        for slot in range(4):
            for n, part in enumerate(parts):
                half = part.blocks // 2
                for k in range(half):
                    position = k + (half if slot < 2 else 0)
                    piece = piece_of(part, me, team, slot % 2 == 1, position)
                    start = pl.multiple_of(piece * rows + part.low, 8)
                    src = flat_ref.at[pl.ds(start, part.size), :]
                    dst = refs[4 * n + slot].at[k]
                    copies.append(pltpu.make_async_copy(src, dst, sems.at[len(copies)]))
                    copies[-1].start()
        for copy in copies:
            copy.wait()

    outs = [
        jax.ShapeDtypeStruct((part.blocks // 2, part.size, LANES), flat.dtype)
        for part in parts
        for _ in range(4)
    ]
    flat_outs = pl.pallas_call(
        body,
        out_shape=outs,
        in_specs=[pl.BlockSpec(memory_space=pl.ANY)],
        out_specs=[pl.BlockSpec(memory_space=pltpu.VMEM)] * len(outs),
        scratch_shapes=[pltpu.SemaphoreType.DMA((2 * sum(part.blocks for part in parts),))],
        compiler_params=pltpu.CompilerParams(vmem_limit_bytes=GATHER_GRANT),
        cost_estimate=pl.CostEstimate(flops=1 << 20, bytes_accessed=1 << 20, transcendentals=0),
        name="gather_pieces",
    )(flat)
    return [flat_outs[4 * n : 4 * n + 4] for n in range(len(parts))]


def scatter_pieces(parts, held, rows, devices):
    def body(*refs):
        me, team = place_index()
        out, sems = refs[-2], refs[-1]
        copies = []
        for n, part in enumerate(parts):
            half = part.blocks // 2
            for slot, (mine, base) in enumerate(((True, 0), (True, half), (False, 0), (False, half))):
                for k in range(half):
                    piece = piece_of(part, me, team, mine, base + k)
                    dst = out.at[pl.ds(pl.multiple_of(piece * rows + part.low, 8), part.size), :]
                    src = refs[4 * n + slot].at[k]
                    copies.append(pltpu.make_async_copy(src, dst, sems.at[len(copies)]))
                    copies[-1].start()
        for copy in copies:
            copy.wait()

    flat = [x for group in held for x in group]
    return pl.pallas_call(
        body,
        out_shape=jax.ShapeDtypeStruct((devices * rows, LANES), flat[0].dtype),
        in_specs=[pl.BlockSpec(memory_space=pltpu.VMEM)] * len(flat),
        out_specs=pl.BlockSpec(memory_space=pl.ANY),
        scratch_shapes=[pltpu.SemaphoreType.DMA((devices * len(parts),))],
        compiler_params=pltpu.CompilerParams(vmem_limit_bytes=8 << 20),
        cost_estimate=pl.CostEstimate(flops=1 << 20, bytes_accessed=1 << 20, transcendentals=0),
        name="scatter_pieces",
    )(*flat)


def shards(gradients, master_params, first_moment, second_moment):
    devices = lax.axis_size("row") * lax.axis_size("col")
    layers = gradients.shape[1]
    bits = devices.bit_length() - 1
    flat = rows_view(gradients[0])
    rows = flat.shape[0] // devices
    parts = parts_of(bits, rows)

    def swap_cores(x):
        return lax.ppermute(x, AXES, [(i, i ^ 1) for i in range(devices)])

    def swap_chips(x, part, step):
        team = [i.bit_count() & 1 for i in range(devices)]
        return lax.ppermute(x, AXES, [(i, i ^ part.mask(team[i], step)) for i in range(devices)])

    def wide(x):
        return x.astype(jnp.float32)

    def narrow(x):
        return x.astype(jnp.bfloat16)

    kept = []
    for give_high, keep_high, give_low, keep_low in gather_pieces(flat, parts, rows):
        high = wide(keep_high) + wide(swap_cores(give_high))
        low = wide(keep_low) + wide(swap_cores(give_low))
        kept.append([high, low])
    sums = [None] * len(parts)
    for n, part in enumerate(parts):
        high, low = kept[n]
        for step in range(part.steps):
            came = wide(swap_chips(narrow(high), part, step))
            half = low.shape[0] // 2
            if half == 0:
                sums[n] = (low + came)[0]
            else:
                high = low[half:] + came[half:]
                low = low[:half] + came[:half]

    state = [rows_view(x) for x in (master_params, first_moment, second_moment)]
    held = []
    for n, part in enumerate(parts):
        new = adam_update(sums[n] / devices, *(x[part.low : part.high] for x in state))
        block = narrow(new[0])[None]
        for step in range(part.steps - 1, 0, -1):
            block = jnp.concatenate([block, swap_chips(block, part, step)], axis=0)
        held.append([block])
    outs = adam_update(jnp.concatenate(sums, axis=0) / devices, *state)
    for n, part in enumerate(parts):
        (block,) = held[n]
        high = swap_chips(block, part, 0)
        if n == 0:
            high, outs = lax.optimization_barrier((high, outs))
        held[n] = (block, high, swap_cores(block), swap_cores(high))
    new_weights = scatter_pieces(parts, held, rows, devices)
    return tuple(layers_view(x, layers) for x in (*outs, new_weights))


def solution(mesh):
    in_specs = (P(AXES, None, None), P(None, AXES), P(None, AXES), P(None, AXES))
    out_specs = (P(None, AXES), P(None, AXES), P(None, AXES), P())
    return jax.shard_map(shards, mesh=mesh, in_specs=in_specs, out_specs=out_specs, check_vma=False)
```

```python
import jax
import jax.numpy as jnp
from jax import lax
from jax.experimental import pallas as pl
from jax.experimental.pallas import tpu as pltpu
from jax.sharding import PartitionSpec as P

beta_one = 0.9
beta_two = 0.95
learn_rate = 0.001
decay_rate = 0.1
epsilon = 1e-08
adam_step = 10.0

AXES = ("row", "col")
LANES = 128
Y, X, Z = 0, 1, 2
SHARES = (0, 8)
GATHER_GRANT = 52 << 20
SUM_ORDERS = (((X, Y, Z), (Y, Z, X)), ((X, Y, Z), (Z, X, Y)))
SPREAD_ORDERS = (((X, Z, Y), (Y, X, Z)), ((Y, X, Z), (Z, Y, X)))


def adam_update(mean_grad, master_params, first_moment, second_moment):
    new_first = beta_one * first_moment + (1.0 - beta_one) * mean_grad
    new_second = beta_two * second_moment + (1.0 - beta_two) * mean_grad * mean_grad
    first_hat = new_first / (1.0 - beta_one**adam_step)
    second_hat = new_second / (1.0 - beta_two**adam_step)
    new_master = master_params - learn_rate * (
        first_hat / (jnp.sqrt(second_hat) + epsilon) + decay_rate * master_params
    )
    return (new_master, new_first, new_second)


def rows_view(x):
    layers, n = x.shape
    return x.reshape(layers, n // LANES, LANES).transpose(1, 0, 2).reshape(-1, LANES)


def layers_view(x, layers):
    return x.reshape(-1, layers, LANES).transpose(1, 0, 2).reshape(layers, -1)


class Part:
    def __init__(self, low, high, orders):
        self.low, self.high, self.orders = low, high, orders
        self.size = high - low
        self.steps = len(orders[0])
        self.blocks = 1 << self.steps

    def mask(self, team, step):
        return 1 << self.orders[team][step] | 1

    def offset(self, team, position):
        bits = 0
        for step in range(self.steps):
            if position >> (self.steps - 1 - step) & 1:
                bits ^= self.mask(team, step)
        return bits


def parts_of(bits, rows, orders):
    rest = list(range(1, bits))
    if bits < 4:
        return [Part(0, rows, (rest, rest[::-1]))]
    tail = rest[3:]
    cuts = [8 * (rows * share // (8 * 16)) for share in SHARES] + [rows]
    return [
        Part(cuts[k], cuts[k + 1], [[rest[i] for i in order] + tail for order in orders[k]])
        for k in range(len(SHARES))
    ]


def place_index():
    devices = lax.axis_size("row") * lax.axis_size("col")
    me = lax.axis_index("row") * lax.axis_size("col") + lax.axis_index("col")
    team = me
    for bit in range(1, devices.bit_length() - 1):
        team = team ^ (me >> bit)
    return me, team & 1


def piece_of(part, me, team, mine, position):
    first, second = part.offset(0, position), part.offset(1, position)
    if not mine:
        first, second = second, first
    return (me if mine else me ^ 1) ^ jnp.where(team == 0, first, second)


def copy_all(pairs, sems):
    copies = [pltpu.make_async_copy(*pair, sems.at[n]) for n, pair in enumerate(pairs)]
    for copy in copies:
        copy.start()
    for copy in copies:
        copy.wait()


def rows_of(part, piece, rows):
    return pl.ds(pl.multiple_of(piece * rows + part.low, 8), part.size)


def gather_pieces(flat, parts, rows, base, grant):
    def body(flat_ref, *refs):
        me, team = place_index()
        pairs = []
        for n, part in enumerate(parts):
            for slot, mine in enumerate((False, True)):
                for k in range(part.blocks // 2):
                    piece = piece_of(part, me, team, mine, base + k)
                    src = flat_ref.at[rows_of(part, piece, rows), :]
                    pairs.append((src, refs[2 * n + slot].at[k]))
        copy_all(pairs, refs[-1])

    outs = [
        jax.ShapeDtypeStruct((part.blocks // 2, part.size, LANES), flat.dtype)
        for part in parts
        for _ in range(2)
    ]
    flat_outs = pl.pallas_call(
        body,
        out_shape=outs,
        in_specs=[pl.BlockSpec(memory_space=pl.ANY)],
        out_specs=[pl.BlockSpec(memory_space=pltpu.VMEM)] * len(outs),
        scratch_shapes=[pltpu.SemaphoreType.DMA((sum(part.blocks for part in parts),))],
        compiler_params=pltpu.CompilerParams(vmem_limit_bytes=grant),
        cost_estimate=pl.CostEstimate(flops=1 << 20, bytes_accessed=1 << 20, transcendentals=0),
        name="gather_pieces",
    )(flat)
    return [flat_outs[2 * n : 2 * n + 2] for n in range(len(parts))]


def scatter_pieces(whole, items, rows, total):
    def body(*refs):
        me, team = place_index()
        pairs = []
        for n, (part, mine, base, held) in enumerate(items):
            for k in range(held.shape[0]):
                piece = piece_of(part, me, team, mine, base + k)
                pairs.append((refs[n].at[k], refs[-2].at[rows_of(part, piece, rows), :]))
        copy_all(pairs, refs[-1])

    blocks = [held for _, _, _, held in items]
    in_specs = [pl.BlockSpec(memory_space=pltpu.VMEM)] * len(blocks)
    args, aliases = blocks, {}
    if whole is not None:
        in_specs.append(pl.BlockSpec(memory_space=pl.ANY))
        aliases = {len(blocks): 0}
        args = blocks + [whole]
    return pl.pallas_call(
        body,
        out_shape=jax.ShapeDtypeStruct((total, LANES), blocks[0].dtype),
        in_specs=in_specs,
        out_specs=pl.BlockSpec(memory_space=pl.ANY),
        scratch_shapes=[pltpu.SemaphoreType.DMA((sum(x.shape[0] for x in blocks),))],
        input_output_aliases=aliases,
        compiler_params=pltpu.CompilerParams(vmem_limit_bytes=8 << 20),
        cost_estimate=pl.CostEstimate(flops=1 << 20, bytes_accessed=1 << 20, transcendentals=0),
        name="scatter_pieces",
    )(*args)


def shards(gradients, master_params, first_moment, second_moment):
    devices = lax.axis_size("row") * lax.axis_size("col")
    layers = gradients.shape[1]
    bits = devices.bit_length() - 1
    flat = rows_view(gradients[0])
    rows = flat.shape[0] // devices
    parts = parts_of(bits, rows, SUM_ORDERS)
    routes = parts_of(bits, rows, SPREAD_ORDERS)

    def swap_cores(x):
        return lax.ppermute(x, AXES, [(i, i ^ 1) for i in range(devices)])

    def swap_chips(x, part, step):
        team = [i.bit_count() & 1 for i in range(devices)]
        return lax.ppermute(x, AXES, [(i, i ^ part.mask(team[i], step)) for i in range(devices)])

    def wide(x):
        return x.astype(jnp.float32)

    def narrow(x):
        return x.astype(jnp.bfloat16)

    upper = parts[0].blocks // 2
    highs = []
    for give, keep in gather_pieces(flat, parts, rows, upper, GATHER_GRANT):
        highs.append(narrow(wide(keep) + wide(swap_cores(give))))
    kept = []
    lows = gather_pieces(flat, parts, rows, 0, GATHER_GRANT)
    for n, (give, keep) in enumerate(lows):
        kept.append([highs[n], wide(keep) + wide(swap_cores(give))])
    sums = [None] * len(parts)
    for n, part in enumerate(parts):
        high, low = kept[n]
        for step in range(part.steps):
            came = wide(swap_chips(narrow(high), part, step))
            half = low.shape[0] // 2
            if half == 0:
                sums[n] = (low + came)[0]
            else:
                high = low[half:] + came[half:]
                low = low[:half] + came[:half]

    state = [rows_view(x) for x in (master_params, first_moment, second_moment)]
    held = []
    for n, part in enumerate(routes):
        new = adam_update(sums[n] / devices, *(x[part.low : part.high] for x in state))
        block = narrow(new[0])[None]
        for step in range(part.steps - 1, 0, -1):
            came = swap_chips(block, part, step)
            block = jnp.concatenate([block, came], axis=0)
        held.append(block)
    outs = adam_update(jnp.concatenate(sums, axis=0) / devices, *state)
    total = devices * rows
    early = [(p, True, 0, x) for p, x in zip(routes, held)]
    early += [(p, False, 0, swap_cores(x)) for p, x in zip(routes, held)]
    new_weights = scatter_pieces(None, early, rows, total)
    for n, part in enumerate(routes):
        high = swap_chips(held[n], part, 0)
        if n == 0:
            high, outs = lax.optimization_barrier((high, outs))
        other = swap_cores(high)
        late = [(part, True, upper, high), (part, False, upper, other)]
        new_weights = scatter_pieces(new_weights, late, rows, total)
    return tuple(layers_view(x, layers) for x in (*outs, new_weights))


def solution(mesh):
    in_specs = (P(AXES, None, None), P(None, AXES), P(None, AXES), P(None, AXES))
    out_specs = (P(None, AXES), P(None, AXES), P(None, AXES), P())
    return jax.shard_map(shards, mesh=mesh, in_specs=in_specs, out_specs=out_specs, check_vma=False)
```

```python
import jax
import jax.numpy as jnp
from jax import lax
from jax.experimental import pallas as pl
from jax.experimental.pallas import tpu as pltpu
from jax.sharding import PartitionSpec as P

beta_one = 0.9
beta_two = 0.95
learn_rate = 0.001
decay_rate = 0.1
epsilon = 1e-08
adam_step = 10.0

AXES = ("row", "col")
LANES = 128
Y, X, Z = 0, 1, 2
SHARES = (0, 8)
GATHER_GRANT = 52 << 20
SUM_ORDERS = (((X, Y, Z), (Y, Z, X)), ((X, Y, Z), (Z, X, Y)))
SPREAD_ORDERS = (((Z, Y, X), (X, Z, Y)), ((Z, Y, X), (Y, Z, X)))


def adam_update(mean_grad, master_params, first_moment, second_moment):
    new_first = beta_one * first_moment + (1.0 - beta_one) * mean_grad
    new_second = beta_two * second_moment + (1.0 - beta_two) * mean_grad * mean_grad
    first_hat = new_first / (1.0 - beta_one**adam_step)
    second_hat = new_second / (1.0 - beta_two**adam_step)
    new_master = master_params - learn_rate * (
        first_hat / (jnp.sqrt(second_hat) + epsilon) + decay_rate * master_params
    )
    return (new_master, new_first, new_second)


def rows_view(x):
    layers, n = x.shape
    return x.reshape(layers, n // LANES, LANES).transpose(1, 0, 2).reshape(-1, LANES)


def layers_view(x, layers):
    return x.reshape(-1, layers, LANES).transpose(1, 0, 2).reshape(layers, -1)


class Part:
    def __init__(self, low, high, orders):
        self.low, self.high, self.orders = low, high, orders
        self.size = high - low
        self.steps = len(orders[0])
        self.blocks = 1 << self.steps

    def mask(self, team, step):
        return 1 << self.orders[team][step] | 1

    def offset(self, team, position):
        bits = 0
        for step in range(self.steps):
            if position >> (self.steps - 1 - step) & 1:
                bits ^= self.mask(team, step)
        return bits


def parts_of(bits, rows, orders):
    rest = list(range(1, bits))
    if bits < 4:
        return [Part(0, rows, (rest, rest[::-1]))]
    tail = rest[3:]
    cuts = [8 * (rows * share // (8 * 16)) for share in SHARES] + [rows]
    return [
        Part(cuts[k], cuts[k + 1], [[rest[i] for i in order] + tail for order in orders[k]])
        for k in range(len(SHARES))
    ]


def place_index():
    devices = lax.axis_size("row") * lax.axis_size("col")
    me = lax.axis_index("row") * lax.axis_size("col") + lax.axis_index("col")
    team = me
    for bit in range(1, devices.bit_length() - 1):
        team = team ^ (me >> bit)
    return me, team & 1


def piece_of(part, me, team, mine, position):
    first, second = part.offset(0, position), part.offset(1, position)
    if not mine:
        first, second = second, first
    return (me if mine else me ^ 1) ^ jnp.where(team == 0, first, second)


def copy_all(pairs, sems):
    copies = [pltpu.make_async_copy(*pair, sems.at[n]) for n, pair in enumerate(pairs)]
    for copy in copies:
        copy.start()
    for copy in copies:
        copy.wait()


def rows_of(part, piece, rows):
    return pl.ds(pl.multiple_of(piece * rows + part.low, 8), part.size)


def gather_pieces(flat, parts, rows, base, grant):
    def body(flat_ref, *refs):
        me, team = place_index()
        pairs = []
        for n, part in enumerate(parts):
            for slot, mine in enumerate((False, True)):
                for k in range(part.blocks // 2):
                    piece = piece_of(part, me, team, mine, base + k)
                    src = flat_ref.at[rows_of(part, piece, rows), :]
                    pairs.append((src, refs[2 * n + slot].at[k]))
        copy_all(pairs, refs[-1])

    outs = [
        jax.ShapeDtypeStruct((part.blocks // 2, part.size, LANES), flat.dtype)
        for part in parts
        for _ in range(2)
    ]
    flat_outs = pl.pallas_call(
        body,
        out_shape=outs,
        in_specs=[pl.BlockSpec(memory_space=pl.ANY)],
        out_specs=[pl.BlockSpec(memory_space=pltpu.VMEM)] * len(outs),
        scratch_shapes=[pltpu.SemaphoreType.DMA((sum(part.blocks for part in parts),))],
        compiler_params=pltpu.CompilerParams(vmem_limit_bytes=grant),
        cost_estimate=pl.CostEstimate(flops=1 << 20, bytes_accessed=1 << 20, transcendentals=0),
        name="gather_pieces",
    )(flat)
    return [flat_outs[2 * n : 2 * n + 2] for n in range(len(parts))]


def scatter_pieces(whole, items, rows, total):
    def body(*refs):
        me, team = place_index()
        pairs = []
        for n, (part, mine, base, held) in enumerate(items):
            for k in range(held.shape[0]):
                piece = piece_of(part, me, team, mine, base + k)
                pairs.append((refs[n].at[k], refs[-2].at[rows_of(part, piece, rows), :]))
        copy_all(pairs, refs[-1])

    blocks = [held for _, _, _, held in items]
    in_specs = [pl.BlockSpec(memory_space=pltpu.VMEM)] * len(blocks)
    args, aliases = blocks, {}
    if whole is not None:
        in_specs.append(pl.BlockSpec(memory_space=pl.ANY))
        aliases = {len(blocks): 0}
        args = blocks + [whole]
    return pl.pallas_call(
        body,
        out_shape=jax.ShapeDtypeStruct((total, LANES), blocks[0].dtype),
        in_specs=in_specs,
        out_specs=pl.BlockSpec(memory_space=pl.ANY),
        scratch_shapes=[pltpu.SemaphoreType.DMA((sum(x.shape[0] for x in blocks),))],
        input_output_aliases=aliases,
        compiler_params=pltpu.CompilerParams(vmem_limit_bytes=8 << 20),
        cost_estimate=pl.CostEstimate(flops=1 << 20, bytes_accessed=1 << 20, transcendentals=0),
        name="scatter_pieces",
    )(*args)


def shards(gradients, master_params, first_moment, second_moment):
    devices = lax.axis_size("row") * lax.axis_size("col")
    layers = gradients.shape[1]
    bits = devices.bit_length() - 1
    flat = rows_view(gradients[0])
    rows = flat.shape[0] // devices
    parts = parts_of(bits, rows, SUM_ORDERS)
    routes = parts_of(bits, rows, SPREAD_ORDERS)

    def swap_cores(x):
        return lax.ppermute(x, AXES, [(i, i ^ 1) for i in range(devices)])

    def swap_chips(x, part, step):
        team = [i.bit_count() & 1 for i in range(devices)]
        return lax.ppermute(x, AXES, [(i, i ^ part.mask(team[i], step)) for i in range(devices)])

    def wide(x):
        return x.astype(jnp.float32)

    def narrow(x):
        return x.astype(jnp.bfloat16)

    upper = parts[0].blocks // 2
    highs = []
    for give, keep in gather_pieces(flat, parts, rows, upper, GATHER_GRANT):
        highs.append(narrow(wide(keep) + wide(swap_cores(give))))
    kept = []
    lows = gather_pieces(flat, parts, rows, 0, GATHER_GRANT)
    for n, (give, keep) in enumerate(lows):
        kept.append([highs[n], wide(keep) + wide(swap_cores(give))])
    sums = [None] * len(parts)
    for n, part in enumerate(parts):
        high, low = kept[n]
        for step in range(part.steps):
            came = wide(swap_chips(narrow(high), part, step))
            half = low.shape[0] // 2
            if half == 0:
                sums[n] = (low + came)[0]
            else:
                high = low[half:] + came[half:]
                low = low[:half] + came[:half]

    state = [rows_view(x) for x in (master_params, first_moment, second_moment)]
    held = []
    for n, part in enumerate(routes):
        new = adam_update(sums[n] / devices, *(x[part.low : part.high] for x in state))
        block = narrow(new[0])[None]
        for step in range(part.steps - 1, 0, -1):
            came = swap_chips(block, part, step)
            block = jnp.concatenate([block, came], axis=0)
        held.append(block)
    outs = adam_update(jnp.concatenate(sums, axis=0) / devices, *state)
    total = devices * rows
    early = [(p, True, 0, x) for p, x in zip(routes, held)]
    for n, part in enumerate(routes):
        early.append((part, False, 0, swap_cores(held[n])))
    new_weights = scatter_pieces(None, early, rows, total)
    for n, part in enumerate(routes):
        high = swap_chips(held[n], part, 0)
        if n == 0:
            high, outs = lax.optimization_barrier((high, outs))
        other = swap_cores(high)
        late = [(part, True, upper, high), (part, False, upper, other)]
        new_weights = scatter_pieces(new_weights, late, rows, total)
    return tuple(layers_view(x, layers) for x in (*outs, new_weights))


def solution(mesh):
    in_specs = (P(AXES, None, None), P(None, AXES), P(None, AXES), P(None, AXES))
    out_specs = (P(None, AXES), P(None, AXES), P(None, AXES), P())
    return jax.shard_map(shards, mesh=mesh, in_specs=in_specs, out_specs=out_specs, check_vma=False)
```
